32 devices in a mesh: zero: 4 (over y, x), width: 2 (over core), site: 4 (over z).
Axes of the slice: x: 2, y: 2, z: 4, core: 2. Of those that a mesh axis runs over, the one named last changes fastest.
Arguments:
- train_query: bfloat16 [28672, 7168], P(('site', 'zero'), 'width'), parts along dimension 0, may hold values from -0.09375 to 0.09375
- low_query: bfloat16 [28672, 64], P(('site', 'zero')), parts along dimension 0, may hold values from -0.0625 to 0.0625
- high_query: bfloat16 [256, 7168], P('site', 'width'), parts along dimension 0, may hold values from -0.75 to 0.75
- train_key: bfloat16 [28672, 7168], P(('site', 'zero'), 'width'), parts along dimension 0, may hold values from -0.09375 to 0.09375
- low_key: bfloat16 [28672, 64], P(('site', 'zero')), parts along dimension 0, may hold values from -0.0625 to 0.0625
- high_key: bfloat16 [256, 7168], P('site', 'width'), parts along dimension 0, may hold values from -0.75 to 0.75
- train_value: bfloat16 [28672, 7168], P(('site', 'zero'), 'width'), parts along dimension 0, may hold values from -0.09375 to 0.09375
- low_value: bfloat16 [28672, 64], P(('site', 'zero')), parts along dimension 0, may hold values from -0.0625 to 0.0625
- high_value: bfloat16 [256, 7168], P('site', 'width'), parts along dimension 0, may hold values from -0.75 to 0.75
- norm_train: float32 [28672], P(('site', 'zero', 'width')), parts along dimension 0, may hold values from 0.25 to 1.75
- norm_step: float32 [28672], P(('site', 'zero', 'width')), parts along dimension 0, may hold values from -0.3 to 0.3
Outputs:
- final_query: bfloat16 [28672, 7168], P('site', ('width', 'zero')), parts along dimension 0
- final_key: bfloat16 [28672, 7168], P('site', ('width', 'zero')), parts along dimension 0
- final_value: bfloat16 [28672, 7168], P('site', ('width', 'zero')), parts along dimension 0
- scale_query: float32 [28672], P(('site', 'width', 'zero')), parts along dimension 0
- scale_key: float32 [28672], P(('site', 'width', 'zero')), parts along dimension 0
- scale_value: float32 [28672], P(('site', 'width', 'zero')), parts along dimension 0
- serve_norm: bfloat16 [28672], P('site'), parts along dimension 0
The draws below stay inside these ranges and needn't reach their ends.
There are 4 independent parts, one for each index of `site`. The reference program is written for one: setup_inputs(seed, part) draws one part's arguments, and reference() takes and returns one part's arrays. A program takes and returns all parts, laid end to end along the dimension named above; each array names one. Nothing has to cross between parts.
All inputs are finite; a program needn't handle non-finite values. Where the reference program divides by a largest or mean magnitude, that divisor is 1e-20 or more.
Results may differ from the reference program's by a relative error of at most 0.01.
Values may be sent and summed in bfloat16 or wider, within the bound.
No kernel may reach another device: no remote copies, remote signals or barrier semaphores. Data moves between devices by JAX's collectives and lax.ppermute only.
A program may use at most 256 MiB of HBM per device.

```python
import jax
import jax.numpy as jnp

D_MODEL = 7168
Q_DIM = 7168
KV_DIM = 7168
RANK = 64


def with_spikes(values, own_key, source, target, shards_of, factor):
    owner, partner = [(jnp.arange(values.shape[position]) // (values.shape[position] // shards_of)).reshape([-1 if axis == position else 1 for axis in range(values.ndim)]) for position in (source, target)]
    chosen = jax.random.permutation(own_key, shards_of)[partner]
    strong = (owner == chosen) | (owner == (partner + shards_of // 2) % shards_of)
    return jnp.where(strong, factor * values, values)


def block_levels(rng, extent, pieces, smallest, high):
    loudness = 1.0
    for position, parts in pieces:
        heights = jax.random.uniform(jax.random.fold_in(jax.random.fold_in(rng, 6), position), (parts,), jnp.float32, smallest / len(pieces), high / len(pieces))
        loudness = loudness * jnp.repeat(jnp.exp(heights), extent[position] // parts).reshape((-1,) + (1,) * (len(extent) - 1 - position))
    return loudness


def scatter_about(key, extent, scale, most, pieces=(), dtype=jnp.bfloat16):
    loudness = block_levels(key, extent, pieces, -0.22, 0.18) if pieces else 1.0
    values = jax.random.normal(key, extent, jnp.float32) * scale * loudness
    return jnp.minimum(jnp.maximum(values, -most), most).astype(dtype)


def gaussian_with(own_key, shape, width, reach, shards, heavy, held_as=jnp.bfloat16):
    array = width * jax.random.normal(own_key, shape, jnp.float32)
    if shards:
        array = array * block_levels(own_key, shape, shards, -0.22, 0.18)
    return jnp.clip(with_spikes(array, jax.random.fold_in(own_key, 3), *heavy), -reach, reach).astype(held_as)


def setup_inputs(seed: int = 0, part: int = 0) -> dict:
    key_list = jax.random.split(jax.random.key(seed), 12)
    own_keys = jax.random.split(jax.random.fold_in(key_list[11], part), 12)
    train_query = gaussian_with(own_keys[0], (D_MODEL, Q_DIM), D_MODEL ** -0.5, 0.09375, ((0, 4), (1, 2)), (0, 1, 4, 2.0))
    low_query = scatter_about(own_keys[1], (D_MODEL, RANK), D_MODEL ** -0.5, 0.0625, ((0, 4),))
    high_query = scatter_about(own_keys[2], (RANK, Q_DIM), RANK ** -0.5, 0.75, ((1, 2),))
    train_key = gaussian_with(own_keys[3], (D_MODEL, KV_DIM), D_MODEL ** -0.5, 0.09375, ((0, 4), (1, 2)), (0, 1, 4, 2.0))
    low_key = scatter_about(own_keys[4], (D_MODEL, RANK), D_MODEL ** -0.5, 0.0625, ((0, 4),))
    high_key = scatter_about(own_keys[5], (RANK, KV_DIM), RANK ** -0.5, 0.75, ((1, 2),))
    train_value = gaussian_with(own_keys[6], (D_MODEL, KV_DIM), D_MODEL ** -0.5, 0.09375, ((0, 4), (1, 2)), (0, 1, 4, 2.0))
    low_value = scatter_about(own_keys[7], (D_MODEL, RANK), D_MODEL ** -0.5, 0.0625, ((0, 4),))
    high_value = scatter_about(own_keys[8], (RANK, KV_DIM), RANK ** -0.5, 0.75, ((1, 2),))
    norm_train = jnp.clip(1.0 + 0.15 * jax.random.normal(own_keys[9], (D_MODEL,), jnp.float32), 0.25, 1.75)
    norm_step = jnp.clip(jax.random.uniform(own_keys[10], (D_MODEL,), jnp.float32, -0.3, 0.3) * block_levels(own_keys[10], (D_MODEL,), ((0, 8),), -0.4, 0.0), -0.3, 0.3)
    return dict(train_query=train_query, low_query=low_query, high_query=high_query, train_key=train_key, low_key=low_key, high_key=high_key, train_value=train_value, low_value=low_value, high_value=high_value, norm_train=norm_train, norm_step=norm_step)


mix_rate = 1.0


def reference(train_query, low_query, high_query, train_key, low_key, high_key, train_value, low_value, high_value, norm_train, norm_step):
    result_query = train_query.astype(jnp.float32) + mix_rate * jnp.dot(low_query, high_query, preferred_element_type=jnp.float32)
    result_key = train_key.astype(jnp.float32) + mix_rate * jnp.dot(low_key, high_key, preferred_element_type=jnp.float32)
    result_value = train_value.astype(jnp.float32) + mix_rate * jnp.dot(low_value, high_value, preferred_element_type=jnp.float32)
    scale_query = jnp.sum(jnp.abs(result_query), axis=0) / D_MODEL
    final_query = (result_query / scale_query).astype(jnp.bfloat16)
    scale_key = jnp.sum(jnp.abs(result_key), axis=0) / D_MODEL
    final_key = (result_key / scale_key).astype(jnp.bfloat16)
    scale_value = jnp.sum(jnp.abs(result_value), axis=0) / D_MODEL
    final_value = (result_value / scale_value).astype(jnp.bfloat16)
    serve_norm = (norm_train + norm_step).astype(jnp.bfloat16)
    return final_query, final_key, final_value, scale_query, scale_key, scale_value, serve_norm
```

```python
import functools

import jax
import jax.numpy as jnp
from jax import lax
from jax.experimental import pallas as pl
from jax.experimental.pallas import tpu as pltpu
from jax.sharding import PartitionSpec as P


mix_rate = 1.0
LANES = 128
ANYWHERE = pl.BlockSpec(memory_space=pl.ANY)


def merged(train_ref, low_ref, high_ref):
    product = lax.dot_general(
        low_ref[...], high_ref[...], (((0,), (0,)), ((), ())), preferred_element_type=jnp.float32
    )
    return train_ref[...].astype(jnp.float32) + mix_rate * product


def add_up(result, sum_ref):
    part = jnp.sum(jnp.abs(result), axis=0, keepdims=True)

    @pl.when(pl.program_id(0) == 0)
    def _():
        sum_ref[...] = part

    @pl.when(pl.program_id(0) > 0)
    def _():
        sum_ref[...] += part


def piece_kernel(place_ref, train_ref, low_ref, high_ref, after_ref, piece_ref, sum_ref):
    result = merged(train_ref, low_ref, high_ref)
    piece_ref[...] = result.astype(piece_ref.dtype)
    add_up(result, sum_ref)


def sum_kernel(place_ref, train_ref, low_ref, high_ref, after_ref, sum_ref):
    add_up(merged(train_ref, low_ref, high_ref), sum_ref)


def own_kernel(place_ref, train_ref, low_ref, high_ref, inverse_ref, after_ref, out_ref):
    out_ref[...] = (merged(train_ref, low_ref, high_ref) * inverse_ref[...]).astype(out_ref.dtype)


def land_kernel(place_ref, piece_ref, inverse_ref, held_ref, out_ref):
    out_ref[...] = (piece_ref[...].astype(jnp.float32) * inverse_ref[...]).astype(out_ref.dtype)


class Matrix:
    def __init__(self, train, low, high, place, parts):
        self.train, self.low, self.high, self.place = train, low.T, high, place
        self.rows, self.rank = low.shape
        self.columns = train.shape[1] // parts
        self.parts = parts
        self.step = 256 if self.rows % 256 == 0 else LANES

    def inputs(self, shift, start):
        first = start // self.step
        return [
            pl.BlockSpec((self.step, self.columns), lambda i, p: (first + i, p[0] ^ shift)),
            pl.BlockSpec((self.rank, self.step), lambda i, p: (0, first + i)),
            pl.BlockSpec((self.rank, self.columns), lambda i, p: (0, p[0] ^ shift)),
        ]

    def call(self, kernel, rows, in_specs, out_specs, out_shape, args, flops, moved, aliases=None):
        return pl.pallas_call(
            kernel,
            grid_spec=pltpu.PrefetchScalarGridSpec(
                num_scalar_prefetch=1,
                grid=(rows // self.step,),
                in_specs=in_specs,
                out_specs=out_specs,
            ),
            out_shape=out_shape,
            input_output_aliases=aliases or {},
            compiler_params=pltpu.CompilerParams(dimension_semantics=("arbitrary",)),
            cost_estimate=pl.CostEstimate(flops=flops, bytes_accessed=moved, transcendentals=0),
        )(self.place, *args)

    def work(self, rows):
        return 2 * rows * self.rank * self.columns

    def piece(self, shift, start, rows, after):
        return self.call(
            piece_kernel,
            rows,
            self.inputs(shift, start) + [ANYWHERE],
            [
                pl.BlockSpec((self.step, self.columns), lambda i, p: (i, 0)),
                pl.BlockSpec((1, self.columns), lambda i, p: (0, 0)),
            ],
            [
                jax.ShapeDtypeStruct((rows, self.columns), self.train.dtype),
                jax.ShapeDtypeStruct((1, self.columns), jnp.float32),
            ],
            (self.train, self.low, self.high, after),
            self.work(rows),
            4 * rows * self.columns,
        )

    def sums(self, after):
        return self.call(
            sum_kernel,
            self.rows,
            self.inputs(0, 0) + [ANYWHERE],
            pl.BlockSpec((1, self.columns), lambda i, p: (0, 0)),
            jax.ShapeDtypeStruct((1, self.columns), jnp.float32),
            (self.train, self.low, self.high, after),
            self.work(self.rows),
            2 * self.rows * self.columns,
        )

    def out_block(self, shift, start):
        blocks, first = self.rows // self.step, start // self.step
        return pl.BlockSpec(
            (self.step, self.columns), lambda i, p: ((p[0] ^ shift) * blocks + first + i, 0)
        )

    def out_shape(self):
        return jax.ShapeDtypeStruct((self.rows * self.parts, self.columns), self.train.dtype)

    def own(self, inverse, after):
        return self.call(
            own_kernel,
            self.rows,
            self.inputs(0, 0) + [pl.BlockSpec((1, self.columns), lambda i, p: (0, 0)), ANYWHERE],
            self.out_block(0, 0),
            self.out_shape(),
            (self.train, self.low, self.high, inverse, after),
            self.work(self.rows),
            4 * self.rows * self.columns,
        )

    def land(self, out, piece, inverse, shift, start):
        rows = piece.shape[0]
        return self.call(
            land_kernel,
            rows,
            [
                pl.BlockSpec((self.step, self.columns), lambda i, p: (i, 0)),
                pl.BlockSpec((1, self.columns), lambda i, p: (0, 0)),
                ANYWHERE,
            ],
            self.out_block(shift, start),
            self.out_shape(),
            (piece, inverse, out),
            self.work(rows),
            4 * rows * self.columns,
            {3: 0},
        )


def ordered(stack, place, axis):
    size = stack.shape[axis]
    bit = 1
    while bit < size:
        at = lax.broadcasted_iota(jnp.int32, stack.shape, axis)
        split = stack.shape[:axis] + (size // (2 * bit), 2, bit) + stack.shape[axis + 1 :]
        turned = jnp.flip(stack.reshape(split), axis + 1).reshape(stack.shape)
        stack = jnp.where((place & bit) + 0 * at > 0, turned, stack)
        bit *= 2
    return stack


def exchange(values, axis, size, shift):
    return lax.ppermute(values, axis, [(i, i ^ shift) for i in range(size)])


def by_permutes(parts, widths, *arguments):
    place = lax.axis_index("zero").astype(jnp.int32)
    place_array = place.reshape(1)
    across = lax.axis_index("width").astype(jnp.int32)
    matrices = [Matrix(*arguments[3 * m : 3 * m + 3], place_array, parts) for m in range(3)]
    norm_train, norm_step = arguments[9:]
    rows, columns = matrices[0].rows, matrices[0].columns
    step = matrices[0].step
    total_rows = rows * parts

    norm = norm_train + norm_step
    norms = [norm] + [exchange(norm, "width", widths, w) for w in range(1, widths)]

    shifts = sorted(range(1, parts), key=lambda k: -bin(k).count("1"))
    last = len(matrices) - 1

    def cuts(m, shift):
        if m == 0 and shift == shifts[0] and rows > step:
            return [(0, step), (step, rows - step)]
        if m == last and shift != shifts[0] and rows > step:
            return [(0, rows - step), (rows - step, step)]
        return [(0, rows)]

    def wire_order(m):
        chunks = [(shift, start, count) for shift in shifts for start, count in cuts(m, shift)]
        return sorted(chunks, key=lambda c: c[1]) if m == last else chunks

    sent, sums = {}, {}
    after = matrices[0].high
    for m, matrix in enumerate(matrices):
        for shift, start, count in wire_order(m):
            sent[m, shift, start], after = matrix.piece(shift, start, count, after)
            sums[m, shift] = sums[m, shift] + after if (m, shift) in sums else after
        if m == 0:
            for other, extra in enumerate(matrices):
                sums[other, 0] = after = extra.sums(after)

    def wire(values, shift):
        return exchange(values, "zero", parts, shift)

    came = {}

    def send(m):
        for shift, start, _ in wire_order(m):
            came[m, shift, start] = wire(sent[m, shift, start], shift)

    send(0)
    small = {}
    for shift in shifts:
        lines = [sums[m, shift] for m in range(len(matrices))] + [n.reshape(1, -1) for n in norms]
        lines += [jnp.zeros_like(lines[0])] * (-len(lines) % 8)
        small[shift] = wire(jnp.concatenate(lines), shift)
    for m in range(1, len(matrices)):
        send(m)

    scales, inverses = [], []
    for m in range(len(matrices)):
        total = sums[m, 0].reshape(columns)
        for shift in shifts:
            total = total + small[shift][m]
        scales.append(total / total_rows)
        inverses.append((1.0 / scales[-1]).reshape(1, columns))

    finals = []
    after = inverses[0]
    for m, matrix in enumerate(matrices):
        out = matrix.own(inverses[m], after)
        for shift, start, _ in wire_order(m):
            out = matrix.land(out, came[m, shift, start], inverses[m], shift, start)
        finals.append(out)
        after = out

    stack = jnp.stack(
        [jnp.stack(norms)]
        + [small[shift][len(matrices) : len(matrices) + widths] for shift in range(1, parts)]
    )
    serve_norm = ordered(ordered(stack, place, 0), across, 1).reshape(-1).astype(jnp.bfloat16)
    return (*finals, *scales, serve_norm)


def by_all_to_all(parts, *arguments):
    finals, scales = [], []
    place = lax.axis_index("zero")
    for m in range(3):
        train, low, high = arguments[3 * m : 3 * m + 3]
        result = train.astype(jnp.float32) + mix_rate * jnp.dot(
            low, high, preferred_element_type=jnp.float32
        )
        total = lax.psum(jnp.sum(jnp.abs(result), axis=0), "zero")
        scale = total / (train.shape[0] * parts)
        narrow = (result / scale).astype(jnp.bfloat16)
        final = lax.all_to_all(narrow, "zero", split_axis=1, concat_axis=0, tiled=True)
        finals.append(final)
        scales.append(lax.dynamic_slice_in_dim(scale, place * final.shape[1], final.shape[1]))
    norm_train, norm_step = arguments[9:]
    serve_norm = lax.all_gather(
        (norm_train + norm_step).astype(jnp.bfloat16), ("zero", "width"), axis=0, tiled=True
    )
    return (*finals, *scales, serve_norm)


def shards(parts, widths, *arguments):
    rows, width = arguments[0].shape
    powers = all(size & (size - 1) == 0 for size in (parts, widths))
    blocks = rows % LANES == 0 and width % (parts * LANES) == 0
    if powers and blocks and 1 < parts <= 8:
        return by_permutes(parts, widths, *arguments)
    return by_all_to_all(parts, *arguments)


def solution(mesh):
    weights = (P(("site", "zero"), "width"), P(("site", "zero"), None), P("site", "width"))
    norms = (P(("site", "zero", "width")),) * 2
    out_specs = (
        (P("site", ("width", "zero")),) * 3 + (P(("site", "width", "zero")),) * 3 + (P("site"),)
    )
    body = functools.partial(shards, mesh.shape["zero"], mesh.shape["width"])
    return jax.shard_map(
        body, mesh=mesh, in_specs=weights * 3 + norms, out_specs=out_specs, check_vma=False
    )
```

```python
import functools

import jax
import jax.numpy as jnp
from jax import lax
from jax.experimental import pallas as pl
from jax.experimental.pallas import tpu as pltpu
from jax.sharding import PartitionSpec as P


mix_rate = 1.0
LANES = 128
VMEM_BYTES = 67043328
ANYWHERE = pl.BlockSpec(memory_space=pl.ANY)


def merged(train_ref, low_ref, high_ref):
    product = lax.dot_general(
        low_ref[...], high_ref[...], (((0,), (0,)), ((), ())), preferred_element_type=jnp.float32
    )
    return train_ref[...].astype(jnp.float32) + mix_rate * product


def add_up(result, before_ref, sum_ref):
    part = jnp.sum(jnp.abs(result), axis=0, keepdims=True)

    @pl.when(pl.program_id(0) == 0)
    def _():
        sum_ref[...] = part if before_ref is None else before_ref[...] + part

    @pl.when(pl.program_id(0) > 0)
    def _():
        sum_ref[...] += part


def piece_kernel(place_ref, train_ref, low_ref, high_ref, after_ref, piece_ref, sum_ref):
    result = merged(train_ref, low_ref, high_ref)
    piece_ref[...] = result.astype(piece_ref.dtype)
    add_up(result, None, sum_ref)


def next_kernel(place_ref, train_ref, low_ref, high_ref, after_ref, before_ref, piece_ref, sum_ref):
    result = merged(train_ref, low_ref, high_ref)
    piece_ref[...] = result.astype(piece_ref.dtype)
    add_up(result, before_ref, sum_ref)


def carry_kernel(sums, place_ref, held_ref, lines_ref, piece_ref):
    lines, rows = lines_ref[...], []
    for i in range(sums):
        line = lines[i : i + 1, :]
        high = line.astype(piece_ref.dtype).astype(jnp.float32)
        rows += [high, line - high]
    count = piece_ref.shape[0]
    rows += [lines[i : i + 1, :] for i in range(sums, sums + count - len(rows))]
    piece_ref[...] = jnp.concatenate(rows, axis=0).astype(piece_ref.dtype)


def sum_kernel(place_ref, train_ref, low_ref, high_ref, after_ref, sum_ref):
    add_up(merged(train_ref, low_ref, high_ref), None, sum_ref)


def own_kernel(place_ref, train_ref, low_ref, high_ref, inverse_ref, after_ref, out_ref):
    out_ref[...] = (merged(train_ref, low_ref, high_ref) * inverse_ref[...]).astype(out_ref.dtype)


def land_kernel(steps, place_ref, inverse_ref, held_ref, *refs):
    *piece_refs, out_ref = refs
    for n, piece_ref in enumerate(piece_refs):

        @pl.when(pl.program_id(0) // steps == n)
        def _():
            out_ref[...] = (piece_ref[...].astype(jnp.float32) * inverse_ref[...]).astype(
                out_ref.dtype
            )


class Matrix:
    def __init__(self, train, low, high, place, parts):
        self.train, self.low, self.high, self.place = train, low.T, high, place
        self.rows, self.rank = low.shape
        self.columns = train.shape[1] // parts
        self.parts = parts
        self.line = pl.BlockSpec((1, self.columns), lambda i, p: (0, 0))

    def step(self, start, rows, at_most=256):
        sizes = [s for s in range(LANES, max(at_most, LANES) + 1, LANES)]
        return max(s for s in sizes if rows % s == 0 and start % s == 0 and self.rows % s == 0)

    def inputs(self, shift, start, step):
        first = start // step
        return [
            pl.BlockSpec((step, self.columns), lambda i, p: (first + i, p[0] ^ shift)),
            pl.BlockSpec((self.rank, step), lambda i, p: (0, first + i)),
            pl.BlockSpec((self.rank, self.columns), lambda i, p: (0, p[0] ^ shift)),
        ]

    def call(self, kernel, steps, in_specs, out_specs, out_shape, args, rows, moved, aliases=None):
        return pl.pallas_call(
            kernel,
            grid_spec=pltpu.PrefetchScalarGridSpec(
                num_scalar_prefetch=1, grid=(steps,), in_specs=in_specs, out_specs=out_specs
            ),
            out_shape=out_shape,
            input_output_aliases=aliases or {},
            compiler_params=pltpu.CompilerParams(
                dimension_semantics=("arbitrary",), vmem_limit_bytes=VMEM_BYTES
            ),
            cost_estimate=pl.CostEstimate(
                flops=2 * rows * self.rank * self.columns, bytes_accessed=moved, transcendentals=0
            ),
        )(self.place, *args)

    def sum_shape(self):
        return jax.ShapeDtypeStruct((1, self.columns), jnp.float32)

    def piece(self, shift, start, rows, after, before=None, extra=0):
        step = self.step(start, rows)
        steps = rows // step
        more = () if before is None else (before,)
        return self.call(
            piece_kernel if before is None else next_kernel,
            steps,
            self.inputs(shift, start, step) + [ANYWHERE] + [self.line] * len(more),
            [pl.BlockSpec((step, self.columns), lambda i, p: (i, 0)), self.line],
            [jax.ShapeDtypeStruct((rows + extra, self.columns), self.train.dtype), self.sum_shape()],
            (self.train, self.low, self.high, after, *more),
            rows,
            4 * rows * self.columns,
        )

    def carry(self, piece, lines, sums, extra):
        return self.call(
            functools.partial(carry_kernel, sums),
            1,
            [ANYWHERE, pl.BlockSpec(lines.shape, lambda i, p: (0, 0))],
            pl.BlockSpec((extra, self.columns), lambda i, p: (piece.shape[0] // extra - 1, 0)),
            jax.ShapeDtypeStruct(piece.shape, piece.dtype),
            (piece, lines),
            extra,
            2 * extra * self.columns,
            {1: 0},
        )

    def sums(self, after):
        step = self.step(0, self.rows)
        return self.call(
            sum_kernel,
            self.rows // step,
            self.inputs(0, 0, step) + [ANYWHERE],
            self.line,
            self.sum_shape(),
            (self.train, self.low, self.high, after),
            self.rows,
            2 * self.rows * self.columns,
        )

    def out_shape(self):
        return jax.ShapeDtypeStruct((self.rows * self.parts, self.columns), self.train.dtype)

    def own(self, inverse, after):
        step = self.step(0, self.rows)
        steps = self.rows // step
        return self.call(
            own_kernel,
            steps,
            self.inputs(0, 0, step) + [self.line, ANYWHERE],
            pl.BlockSpec((step, self.columns), lambda i, p: (p[0] * steps + i, 0)),
            self.out_shape(),
            (self.train, self.low, self.high, inverse, after),
            self.rows,
            4 * self.rows * self.columns,
        )

    def land(self, out, pieces, inverse, shifts, start, rows):
        step = self.step(start, rows, 384)
        steps, blocks, first = rows // step, self.rows // step, start // step

        def source(n):
            return lambda i, p: (jnp.clip(i - n * steps, 0, steps - 1), 0)

        def target(i, p):
            shift = shifts[0]
            for n in range(1, len(shifts)):
                shift = jnp.where(i // steps == n, shifts[n], shift)
            return ((p[0] ^ shift) * blocks + first + i % steps, 0)

        return self.call(
            functools.partial(land_kernel, steps),
            steps * len(pieces),
            [self.line, ANYWHERE]
            + [pl.BlockSpec((step, self.columns), source(n)) for n in range(len(pieces))],
            pl.BlockSpec((step, self.columns), target),
            self.out_shape(),
            (inverse, out, *pieces),
            rows * len(pieces),
            4 * rows * len(pieces) * self.columns,
            {2: 0},
        )


def ordered(stack, place, axis):
    size = stack.shape[axis]
    bit = 1
    while bit < size:
        at = lax.broadcasted_iota(jnp.int32, stack.shape, axis)
        split = stack.shape[:axis] + (size // (2 * bit), 2, bit) + stack.shape[axis + 1 :]
        turned = jnp.flip(stack.reshape(split), axis + 1).reshape(stack.shape)
        stack = jnp.where((place & bit) + 0 * at > 0, turned, stack)
        bit *= 2
    return stack


def exchange(values, axis, size, shift):
    return lax.ppermute(values, axis, [(i, i ^ shift) for i in range(size)])


def cuts_of(rows, sizes):
    known = sum(size or 0 for size in sizes)
    if rows <= known:
        return [(0, rows)]
    counts = [size or rows - known for size in sizes]
    return [(sum(counts[:n]), count) for n, count in enumerate(counts)]


def by_permutes(parts, widths, *arguments):
    place = lax.axis_index("zero").astype(jnp.int32)
    place_array = place.reshape(1)
    across = lax.axis_index("width").astype(jnp.int32)
    matrices = [Matrix(*arguments[3 * m : 3 * m + 3], place_array, parts) for m in range(3)]
    norm_train, norm_step = arguments[9:]
    rows, columns = matrices[0].rows, matrices[0].columns
    total_rows = rows * parts

    shifts = sorted(range(1, parts), key=lambda k: -bin(k).count("1"))
    far, near = shifts[:1], shifts[1:]
    first, carrier, last = 0, 1, 2

    whole = cuts_of(rows, [None])
    messages = {
        first: [(cut, far) for cut in cuts_of(rows, [256, None])] + [(whole[0], near)],
        carrier: [(whole[0], shifts)],
        last: [(whole[0], far)] + [(cut, near) for cut in cuts_of(rows, [None, 384, 128])],
    }

    def wire(values, shift):
        return exchange(values, "zero", parts, shift)

    norm = norm_train + norm_step
    norms = [norm] + [exchange(norm, "width", widths, w) for w in range(1, widths)]
    norms = jnp.stack(norms)

    at = 2 * len(matrices)
    extra = -(-(at + widths) // 8) * 8
    sent, sums = {}, {}
    after = matrices[0].high

    def pieces(m, carry=False):
        nonlocal after
        for (start, count), group in messages[m]:
            for shift in group:
                sent[m, shift, start], after = matrices[m].piece(
                    shift, start, count, after, sums.get((m, shift)), extra if carry else 0
                )
                sums[m, shift] = after
                if carry:
                    lines = [sums[o, shift] for o in range(len(matrices))] + [norms]
                    lines += [jnp.zeros((extra - len(matrices) - widths, columns), jnp.float32)]
                    sent[m, shift, start] = matrices[m].carry(
                        sent[m, shift, start], jnp.concatenate(lines), len(matrices), extra
                    )

    pieces(first)
    for m, matrix in enumerate(matrices):
        sums[m, 0] = after = matrix.sums(after)
    pieces(last)
    pieces(carrier, True)

    came = {}
    for m in (first, carrier, last):
        for (start, count), group in messages[m]:
            for shift in group:
                came[m, shift, start] = wire(sent[m, shift, start], shift)

    small = {shift: came[carrier, shift, 0][rows:].astype(jnp.float32) for shift in shifts}
    scales, inverses = [], []
    for m in range(len(matrices)):
        total = sums[m, 0].reshape(columns)
        for shift in shifts:
            total = total + (small[shift][2 * m] + small[shift][2 * m + 1])
        scales.append(total / total_rows)
        inverses.append((1.0 / scales[-1]).reshape(1, columns))

    stack = jnp.stack(
        [norms] + [small[shift][at : at + widths] for shift in range(1, parts)]
    )
    serve_norm = ordered(ordered(stack, place, 0), across, 1).reshape(-1).astype(jnp.bfloat16)

    finals = {}
    after = serve_norm
    for m in (first, carrier, last):
        out = matrices[m].own(inverses[m], after)
        for (start, count), group in messages[m]:
            batches = [group] if m == last else [[shift] for shift in group]
            for batch in batches:
                arrived = [came[m, shift, start] for shift in batch]
                out = matrices[m].land(out, arrived, inverses[m], batch, start, count)
        finals[m] = after = out

    return (finals[0], finals[1], finals[2], *scales, serve_norm)


def by_all_to_all(parts, *arguments):
    finals, scales = [], []
    place = lax.axis_index("zero")
    for m in range(3):
        train, low, high = arguments[3 * m : 3 * m + 3]
        result = train.astype(jnp.float32) + mix_rate * jnp.dot(
            low, high, preferred_element_type=jnp.float32
        )
        total = lax.psum(jnp.sum(jnp.abs(result), axis=0), "zero")
        scale = total / (train.shape[0] * parts)
        narrow = (result / scale).astype(jnp.bfloat16)
        final = lax.all_to_all(narrow, "zero", split_axis=1, concat_axis=0, tiled=True)
        finals.append(final)
        scales.append(lax.dynamic_slice_in_dim(scale, place * final.shape[1], final.shape[1]))
    norm_train, norm_step = arguments[9:]
    serve_norm = lax.all_gather(
        (norm_train + norm_step).astype(jnp.bfloat16), ("zero", "width"), axis=0, tiled=True
    )
    return (*finals, *scales, serve_norm)


def shards(parts, widths, *arguments):
    rows, width = arguments[0].shape
    powers = all(size & (size - 1) == 0 for size in (parts, widths))
    blocks = rows % LANES == 0 and widths <= 8 and width % (parts * LANES) == 0
    if powers and blocks and 1 < parts <= 8:
        return by_permutes(parts, widths, *arguments)
    return by_all_to_all(parts, *arguments)


def solution(mesh):
    weights = (P(("site", "zero"), "width"), P(("site", "zero"), None), P("site", "width"))
    norms = (P(("site", "zero", "width")),) * 2
    out_specs = (
        (P("site", ("width", "zero")),) * 3 + (P(("site", "width", "zero")),) * 3 + (P("site"),)
    )
    body = functools.partial(shards, mesh.shape["zero"], mesh.shape["width"])
    return jax.shard_map(
        body, mesh=mesh, in_specs=weights * 3 + norms, out_specs=out_specs, check_vma=False
    )
```

```python
import functools

import jax
import jax.numpy as jnp
from jax import lax
from jax.experimental import pallas as pl
from jax.experimental.pallas import tpu as pltpu
from jax.sharding import PartitionSpec as P


mix_rate = 1.0
LANES = 128
VMEM_BYTES = 67043328
ANYWHERE = pl.BlockSpec(memory_space=pl.ANY)


def merge_rows(train_ref, low_ref, high_ref, use):
    count, columns = train_ref.shape
    few = 256 if count % 256 == 0 else LANES

    def some(j, part):
        rows = pl.ds(pl.multiple_of(j * few, few), few)
        product = lax.dot_general(
            low_ref[:, rows],
            high_ref[...],
            (((0,), (0,)), ((), ())),
            preferred_element_type=jnp.float32,
        )
        result = train_ref[rows, :].astype(jnp.float32) + mix_rate * product
        use(rows, result)
        return part + jnp.sum(jnp.abs(result).reshape(few // 8, 8, columns), axis=0)

    return lax.fori_loop(0, count // few, some, jnp.zeros((8, columns), jnp.float32))


def add_up(part, before_ref, sum_ref):
    part = jnp.sum(part, axis=0, keepdims=True)

    @pl.when(pl.program_id(0) == 0)
    def _():
        sum_ref[...] = part if before_ref is None else before_ref[...] + part

    @pl.when(pl.program_id(0) > 0)
    def _():
        sum_ref[...] += part


def piece_kernel(place_ref, train_ref, low_ref, high_ref, after_ref, *refs):
    *before, piece_ref, sum_ref = refs

    def use(rows, result):
        piece_ref[rows, :] = result.astype(piece_ref.dtype)

    part = merge_rows(train_ref, low_ref, high_ref, use)
    add_up(part, before[0] if before else None, sum_ref)


def carry_kernel(sums, place_ref, held_ref, lines_ref, piece_ref):
    lines, rows = lines_ref[...], []
    for i in range(sums):
        line = lines[i : i + 1, :]
        high = line.astype(piece_ref.dtype).astype(jnp.float32)
        rows += [high, line - high]
    count = piece_ref.shape[0]
    rows += [lines[i : i + 1, :] for i in range(sums, sums + count - len(rows))]
    piece_ref[...] = jnp.concatenate(rows, axis=0).astype(piece_ref.dtype)


def sum_kernel(place_ref, train_ref, low_ref, high_ref, after_ref, sum_ref):
    add_up(merge_rows(train_ref, low_ref, high_ref, lambda rows, result: None), None, sum_ref)


def own_kernel(place_ref, train_ref, low_ref, high_ref, inverse_ref, after_ref, out_ref):
    def use(rows, result):
        out_ref[rows, :] = (result * inverse_ref[...]).astype(out_ref.dtype)

    merge_rows(train_ref, low_ref, high_ref, use)


def land_kernel(steps, place_ref, inverse_ref, held_ref, *refs):
    *piece_refs, out_ref = refs
    count = out_ref.shape[0]
    few = 256 if count % 256 == 0 else LANES
    for n, piece_ref in enumerate(piece_refs):

        @pl.when(pl.program_id(0) // steps == n)
        def _():
            @pl.loop(0, count // few)
            def _(j):
                rows = pl.ds(pl.multiple_of(j * few, few), few)
                out_ref[rows, :] = (
                    piece_ref[rows, :].astype(jnp.float32) * inverse_ref[...]
                ).astype(out_ref.dtype)


class Matrix:
    def __init__(self, train, low, high, place, parts):
        self.train, self.low, self.high, self.place = train, low.T, high, place
        self.rows, self.rank = low.shape
        self.columns = train.shape[1] // parts
        self.parts = parts
        self.line = pl.BlockSpec((1, self.columns), lambda i, p: (0, 0))

    def step(self, start, rows, at_most=896):
        sizes = [s for s in range(LANES, max(at_most, LANES) + 1, LANES)]
        return max(s for s in sizes if rows % s == 0 and start % s == 0 and self.rows % s == 0)

    def inputs(self, shift, start, step):
        first = start // step
        return [
            pl.BlockSpec((step, self.columns), lambda i, p: (first + i, p[0] ^ shift)),
            pl.BlockSpec((self.rank, step), lambda i, p: (0, first + i)),
            pl.BlockSpec((self.rank, self.columns), lambda i, p: (0, p[0] ^ shift)),
        ]

    def call(self, kernel, steps, in_specs, out_specs, out_shape, args, rows, moved, aliases=None):
        return pl.pallas_call(
            kernel,
            grid_spec=pltpu.PrefetchScalarGridSpec(
                num_scalar_prefetch=1, grid=(steps,), in_specs=in_specs, out_specs=out_specs
            ),
            out_shape=out_shape,
            input_output_aliases=aliases or {},
            compiler_params=pltpu.CompilerParams(
                dimension_semantics=("arbitrary",), vmem_limit_bytes=VMEM_BYTES
            ),
            cost_estimate=pl.CostEstimate(
                flops=2 * rows * self.rank * self.columns, bytes_accessed=moved, transcendentals=0
            ),
        )(self.place, *args)

    def sum_shape(self):
        return jax.ShapeDtypeStruct((1, self.columns), jnp.float32)

    def piece(self, shift, start, rows, after, before=None, extra=0):
        step = self.step(start, rows)
        steps = rows // step
        more = () if before is None else (before,)
        return self.call(
            piece_kernel,
            steps,
            self.inputs(shift, start, step) + [ANYWHERE] + [self.line] * len(more),
            [pl.BlockSpec((step, self.columns), lambda i, p: (i, 0)), self.line],
            [jax.ShapeDtypeStruct((rows + extra, self.columns), self.train.dtype), self.sum_shape()],
            (self.train, self.low, self.high, after, *more),
            rows,
            4 * rows * self.columns,
        )

    def carry(self, piece, lines, sums, extra):
        return self.call(
            functools.partial(carry_kernel, sums),
            1,
            [ANYWHERE, pl.BlockSpec(lines.shape, lambda i, p: (0, 0))],
            pl.BlockSpec((extra, self.columns), lambda i, p: (piece.shape[0] // extra - 1, 0)),
            jax.ShapeDtypeStruct(piece.shape, piece.dtype),
            (piece, lines),
            extra,
            2 * extra * self.columns,
            {1: 0},
        )

    def sums(self, after):
        step = self.step(0, self.rows)
        return self.call(
            sum_kernel,
            self.rows // step,
            self.inputs(0, 0, step) + [ANYWHERE],
            self.line,
            self.sum_shape(),
            (self.train, self.low, self.high, after),
            self.rows,
            2 * self.rows * self.columns,
        )

    def out_shape(self):
        return jax.ShapeDtypeStruct((self.rows * self.parts, self.columns), self.train.dtype)

    def own(self, inverse, after):
        step = self.step(0, self.rows)
        steps = self.rows // step
        return self.call(
            own_kernel,
            steps,
            self.inputs(0, 0, step) + [self.line, ANYWHERE],
            pl.BlockSpec((step, self.columns), lambda i, p: (p[0] * steps + i, 0)),
            self.out_shape(),
            (self.train, self.low, self.high, inverse, after),
            self.rows,
            4 * self.rows * self.columns,
        )

    def land(self, out, pieces, inverse, shifts, start, rows):
        step = self.step(start, rows)
        steps, blocks, first = rows // step, self.rows // step, start // step

        def source(n):
            return lambda i, p: (jnp.clip(i - n * steps, 0, steps - 1), 0)

        def target(i, p):
            shift = shifts[0]
            for n in range(1, len(shifts)):
                shift = jnp.where(i // steps == n, shifts[n], shift)
            return ((p[0] ^ shift) * blocks + first + i % steps, 0)

        return self.call(
            functools.partial(land_kernel, steps),
            steps * len(pieces),
            [self.line, ANYWHERE]
            + [pl.BlockSpec((step, self.columns), source(n)) for n in range(len(pieces))],
            pl.BlockSpec((step, self.columns), target),
            self.out_shape(),
            (inverse, out, *pieces),
            rows * len(pieces),
            4 * rows * len(pieces) * self.columns,
            {2: 0},
        )


def ordered(stack, place, axis):
    size = stack.shape[axis]
    bit = 1
    while bit < size:
        at = lax.broadcasted_iota(jnp.int32, stack.shape, axis)
        split = stack.shape[:axis] + (size // (2 * bit), 2, bit) + stack.shape[axis + 1 :]
        turned = jnp.flip(stack.reshape(split), axis + 1).reshape(stack.shape)
        stack = jnp.where((place & bit) + 0 * at > 0, turned, stack)
        bit *= 2
    return stack


def exchange(values, axis, size, shift):
    return lax.ppermute(values, axis, [(i, i ^ shift) for i in range(size)])


def cuts_of(rows, sizes):
    known = sum(size or 0 for size in sizes)
    if rows <= known:
        return [(0, rows)]
    counts = [size or rows - known for size in sizes]
    return [(sum(counts[:n]), count) for n, count in enumerate(counts)]


def by_permutes(parts, widths, *arguments):
    place = lax.axis_index("zero").astype(jnp.int32)
    place_array = place.reshape(1)
    across = lax.axis_index("width").astype(jnp.int32)
    matrices = [Matrix(*arguments[3 * m : 3 * m + 3], place_array, parts) for m in range(3)]
    norm_train, norm_step = arguments[9:]
    rows, columns = matrices[0].rows, matrices[0].columns
    total_rows = rows * parts

    shifts = sorted(range(1, parts), key=lambda k: -bin(k).count("1"))
    far, near = shifts[:1], shifts[1:]
    first, carrier, last = 0, 1, 2

    whole = cuts_of(rows, [None])
    messages = {
        first: [(cut, far) for cut in cuts_of(rows, [256, None])] + [(whole[0], near)],
        carrier: [(whole[0], shifts)],
        last: [(whole[0], far)] + [(cut, near) for cut in cuts_of(rows, [None, 384, 128])],
    }

    def wire(values, shift):
        return exchange(values, "zero", parts, shift)

    norm = norm_train + norm_step
    norms = [norm] + [exchange(norm, "width", widths, w) for w in range(1, widths)]
    norms = jnp.stack(norms)

    at = 2 * len(matrices)
    extra = -(-(at + widths) // 8) * 8
    sent, sums = {}, {}
    after = matrices[0].high

    def pieces(m, carry=False):
        nonlocal after
        for (start, count), group in messages[m]:
            for shift in group:
                sent[m, shift, start], after = matrices[m].piece(
                    shift, start, count, after, sums.get((m, shift)), extra if carry else 0
                )
                sums[m, shift] = after
                if carry:
                    lines = [sums[o, shift] for o in range(len(matrices))] + [norms]
                    lines += [jnp.zeros((extra - len(matrices) - widths, columns), jnp.float32)]
                    sent[m, shift, start] = matrices[m].carry(
                        sent[m, shift, start], jnp.concatenate(lines), len(matrices), extra
                    )

    pieces(first)
    for m, matrix in enumerate(matrices):
        sums[m, 0] = after = matrix.sums(after)
    pieces(last)
    pieces(carrier, True)

    came = {}
    for m in (first, carrier, last):
        for (start, count), group in messages[m]:
            for shift in group:
                came[m, shift, start] = wire(sent[m, shift, start], shift)

    small = {shift: came[carrier, shift, 0][rows:].astype(jnp.float32) for shift in shifts}
    scales, inverses = [], []
    for m in range(len(matrices)):
        total = sums[m, 0].reshape(columns)
        for shift in shifts:
            total = total + (small[shift][2 * m] + small[shift][2 * m + 1])
        scales.append(total / total_rows)
        inverses.append((1.0 / scales[-1]).reshape(1, columns))

    stack = jnp.stack(
        [norms] + [small[shift][at : at + widths] for shift in range(1, parts)]
    )
    serve_norm = ordered(ordered(stack, place, 0), across, 1).reshape(-1).astype(jnp.bfloat16)

    finals = {}
    after = serve_norm
    for m in (first, carrier, last):
        out = matrices[m].own(inverses[m], after)
        for (start, count), group in messages[m]:
            batches = [group] if m == last else [[shift] for shift in group]
            for batch in batches:
                arrived = [came[m, shift, start] for shift in batch]
                out = matrices[m].land(out, arrived, inverses[m], batch, start, count)
        finals[m] = after = out

    return (finals[0], finals[1], finals[2], *scales, serve_norm)


def by_all_to_all(parts, *arguments):
    finals, scales = [], []
    place = lax.axis_index("zero")
    for m in range(3):
        train, low, high = arguments[3 * m : 3 * m + 3]
        result = train.astype(jnp.float32) + mix_rate * jnp.dot(
            low, high, preferred_element_type=jnp.float32
        )
        total = lax.psum(jnp.sum(jnp.abs(result), axis=0), "zero")
        scale = total / (train.shape[0] * parts)
        narrow = (result / scale).astype(jnp.bfloat16)
        final = lax.all_to_all(narrow, "zero", split_axis=1, concat_axis=0, tiled=True)
        finals.append(final)
        scales.append(lax.dynamic_slice_in_dim(scale, place * final.shape[1], final.shape[1]))
    norm_train, norm_step = arguments[9:]
    serve_norm = lax.all_gather(
        (norm_train + norm_step).astype(jnp.bfloat16), ("zero", "width"), axis=0, tiled=True
    )
    return (*finals, *scales, serve_norm)


def shards(parts, widths, *arguments):
    rows, width = arguments[0].shape
    powers = all(size & (size - 1) == 0 for size in (parts, widths))
    blocks = rows % LANES == 0 and widths <= 8 and width % (parts * LANES) == 0
    if powers and blocks and 1 < parts <= 8:
        return by_permutes(parts, widths, *arguments)
    return by_all_to_all(parts, *arguments)


def solution(mesh):
    weights = (P(("site", "zero"), "width"), P(("site", "zero"), None), P("site", "width"))
    norms = (P(("site", "zero", "width")),) * 2
    out_specs = (
        (P("site", ("width", "zero")),) * 3 + (P(("site", "width", "zero")),) * 3 + (P("site"),)
    )
    body = functools.partial(shards, mesh.shape["zero"], mesh.shape["width"])
    return jax.shard_map(
        body, mesh=mesh, in_specs=weights * 3 + norms, out_specs=out_specs, check_vma=False
    )
```

```python
import functools

import jax
import jax.numpy as jnp
from jax import lax
from jax.experimental import pallas as pl
from jax.experimental.pallas import tpu as pltpu
from jax.sharding import PartitionSpec as P


mix_rate = 1.0
LANES = 128
VMEM_BYTES = 67043328
ANYWHERE = pl.BlockSpec(memory_space=pl.ANY)


def merge_rows(train_ref, low_ref, high_ref, use):
    count, columns = train_ref.shape
    few = 256 if count % 256 == 0 else LANES

    def some(j, part):
        rows = pl.ds(pl.multiple_of(j * few, few), few)
        product = lax.dot_general(
            low_ref[:, rows],
            high_ref[...],
            (((0,), (0,)), ((), ())),
            preferred_element_type=jnp.float32,
        )
        result = train_ref[rows, :].astype(jnp.float32) + mix_rate * product
        use(rows, result)
        return part + jnp.sum(jnp.abs(result).reshape(few // 8, 8, columns), axis=0)

    return lax.fori_loop(0, count // few, some, jnp.zeros((8, columns), jnp.float32))


def add_up(part, before_ref, sum_ref):
    part = jnp.sum(part, axis=0, keepdims=True)

    @pl.when(pl.program_id(0) == 0)
    def _():
        sum_ref[...] = part if before_ref is None else before_ref[...] + part

    @pl.when(pl.program_id(0) > 0)
    def _():
        sum_ref[...] += part


def piece_kernel(place_ref, train_ref, low_ref, high_ref, after_ref, *refs):
    *before, piece_ref, sum_ref = refs

    def use(rows, result):
        piece_ref[rows, :] = result.astype(piece_ref.dtype)

    part = merge_rows(train_ref, low_ref, high_ref, use)
    add_up(part, before[0] if before else None, sum_ref)


def carry_kernel(sums, place_ref, held_ref, lines_ref, piece_ref):
    lines, rows = lines_ref[...], []
    for i in range(sums):
        line = lines[i : i + 1, :]
        high = line.astype(piece_ref.dtype).astype(jnp.float32)
        rows += [high, line - high]
    count = piece_ref.shape[0]
    rows += [lines[i : i + 1, :] for i in range(sums, sums + count - len(rows))]
    piece_ref[...] = jnp.concatenate(rows, axis=0).astype(piece_ref.dtype)


def sum_kernel(place_ref, train_ref, low_ref, high_ref, after_ref, sum_ref):
    add_up(merge_rows(train_ref, low_ref, high_ref, lambda rows, result: None), None, sum_ref)


def place_rows(piece_ref, inverse_ref, out_ref):
    count = out_ref.shape[0]
    few = 256 if count % 256 == 0 else LANES

    @pl.loop(0, count // few)
    def _(j):
        rows = pl.ds(pl.multiple_of(j * few, few), few)
        scaled = piece_ref[rows, :].astype(jnp.float32) * inverse_ref[...]
        out_ref[rows, :] = scaled.astype(out_ref.dtype)


def own_kernel(steps, place_ref, train_ref, low_ref, high_ref, inverse_ref, after_ref, *refs):
    *piece_refs, out_ref = refs

    def use(rows, result):
        out_ref[rows, :] = (result * inverse_ref[...]).astype(out_ref.dtype)

    @pl.when(pl.program_id(0) < steps)
    def _():
        merge_rows(train_ref, low_ref, high_ref, use)

    for n, piece_ref in enumerate(piece_refs):

        @pl.when(pl.program_id(0) // steps == n + 1)
        def _():
            place_rows(piece_ref, inverse_ref, out_ref)


def land_kernel(steps, place_ref, inverse_ref, held_ref, *refs):
    *piece_refs, out_ref = refs
    for n, piece_ref in enumerate(piece_refs):

        @pl.when(pl.program_id(0) // steps == n)
        def _():
            place_rows(piece_ref, inverse_ref, out_ref)


class Matrix:
    def __init__(self, train, low, high, place, parts):
        self.train, self.low, self.high, self.place = train, low.T, high, place
        self.rows, self.rank = low.shape
        self.columns = train.shape[1] // parts
        self.parts = parts
        self.line = pl.BlockSpec((1, self.columns), lambda i, p: (0, 0))

    def step(self, rows, at_most=896):
        return max(s for s in range(LANES, at_most + 1, LANES) if rows % s == 0)

    def inputs(self, shift, start, step, steps):
        def at(i):
            return pl.multiple_of(start + jnp.minimum(i, steps - 1) * step, LANES)

        return [
            pl.BlockSpec(
                (pl.Element(step), pl.Element(self.columns)),
                lambda i, p: (at(i), pl.multiple_of((p[0] ^ shift) * self.columns, LANES)),
            ),
            pl.BlockSpec((pl.Element(self.rank), pl.Element(step)), lambda i, p: (0, at(i))),
            pl.BlockSpec((self.rank, self.columns), lambda i, p: (0, p[0] ^ shift)),
        ]

    def call(self, kernel, steps, in_specs, out_specs, out_shape, args, rows, moved, aliases=None):
        return pl.pallas_call(
            kernel,
            grid_spec=pltpu.PrefetchScalarGridSpec(
                num_scalar_prefetch=1, grid=(steps,), in_specs=in_specs, out_specs=out_specs
            ),
            out_shape=out_shape,
            input_output_aliases=aliases or {},
            compiler_params=pltpu.CompilerParams(
                dimension_semantics=("arbitrary",), vmem_limit_bytes=VMEM_BYTES
            ),
            cost_estimate=pl.CostEstimate(
                flops=2 * rows * self.rank * self.columns, bytes_accessed=moved, transcendentals=0
            ),
        )(self.place, *args)

    def sum_shape(self):
        return jax.ShapeDtypeStruct((1, self.columns), jnp.float32)

    def piece(self, shift, start, rows, after, before=None, extra=0):
        step = self.step(rows)
        steps = rows // step
        more = () if before is None else (before,)
        return self.call(
            piece_kernel,
            steps,
            self.inputs(shift, start, step, steps) + [ANYWHERE] + [self.line] * len(more),
            [pl.BlockSpec((step, self.columns), lambda i, p: (i, 0)), self.line],
            [jax.ShapeDtypeStruct((rows + extra, self.columns), self.train.dtype), self.sum_shape()],
            (self.train, self.low, self.high, after, *more),
            rows,
            4 * rows * self.columns,
        )

    def carry(self, piece, lines, sums, extra):
        return self.call(
            functools.partial(carry_kernel, sums),
            1,
            [ANYWHERE, pl.BlockSpec(lines.shape, lambda i, p: (0, 0))],
            pl.BlockSpec((extra, self.columns), lambda i, p: (piece.shape[0] // extra - 1, 0)),
            jax.ShapeDtypeStruct(piece.shape, piece.dtype),
            (piece, lines),
            extra,
            2 * extra * self.columns,
            {1: 0},
        )

    def sums(self, after):
        step = self.step(self.rows)
        return self.call(
            sum_kernel,
            self.rows // step,
            self.inputs(0, 0, step, self.rows // step) + [ANYWHERE],
            self.line,
            self.sum_shape(),
            (self.train, self.low, self.high, after),
            self.rows,
            2 * self.rows * self.columns,
        )

    def out_shape(self):
        return jax.ShapeDtypeStruct((self.rows * self.parts, self.columns), self.train.dtype)

    def source(self, n, steps, step):
        return pl.BlockSpec(
            (step, self.columns), lambda i, p: (jnp.clip(i - n * steps, 0, steps - 1), 0)
        )

    def target(self, shifts, start, steps, step):
        def at(i, p):
            shift = shifts[0]
            for n in range(1, len(shifts)):
                shift = jnp.where(i // steps == n, shifts[n], shift)
            row = (p[0] ^ shift) * self.rows + start + lax.rem(i, steps) * step
            return (pl.multiple_of(row, LANES), 0)

        return pl.BlockSpec((pl.Element(step), pl.Element(self.columns)), at)

    def own(self, inverse, after, pieces=(), shifts=()):
        step = self.step(self.rows)
        steps = self.rows // step
        total = self.rows * (1 + len(pieces))
        return self.call(
            functools.partial(own_kernel, steps),
            steps * (1 + len(pieces)),
            self.inputs(0, 0, step, steps)
            + [self.line, ANYWHERE]
            + [self.source(n + 1, steps, step) for n in range(len(pieces))],
            self.target([0, *shifts], 0, steps, step),
            self.out_shape(),
            (self.train, self.low, self.high, inverse, after, *pieces),
            total,
            4 * total * self.columns,
        )

    def land(self, out, pieces, inverse, shifts, start, rows):
        step = self.step(rows)
        steps = rows // step
        return self.call(
            functools.partial(land_kernel, steps),
            steps * len(pieces),
            [self.line, ANYWHERE]
            + [self.source(n, steps, step) for n in range(len(pieces))],
            self.target(shifts, start, steps, step),
            self.out_shape(),
            (inverse, out, *pieces),
            rows * len(pieces),
            4 * rows * len(pieces) * self.columns,
            {2: 0},
        )


def ordered(stack, place, axis):
    size = stack.shape[axis]
    bit = 1
    while bit < size:
        at = lax.broadcasted_iota(jnp.int32, stack.shape, axis)
        split = stack.shape[:axis] + (size // (2 * bit), 2, bit) + stack.shape[axis + 1 :]
        turned = jnp.flip(stack.reshape(split), axis + 1).reshape(stack.shape)
        stack = jnp.where((place & bit) + 0 * at > 0, turned, stack)
        bit *= 2
    return stack


def exchange(values, axis, size, shift):
    return lax.ppermute(values, axis, [(i, i ^ shift) for i in range(size)])


def cuts_of(rows, sizes):
    known = sum(size or 0 for size in sizes)
    if rows <= known:
        return [(0, rows)]
    counts = [size or rows - known for size in sizes]
    return [(sum(counts[:n]), count) for n, count in enumerate(counts)]


def by_permutes(parts, widths, *arguments):
    place = lax.axis_index("zero").astype(jnp.int32)
    place_array = place.reshape(1)
    across = lax.axis_index("width").astype(jnp.int32)
    matrices = [Matrix(*arguments[3 * m : 3 * m + 3], place_array, parts) for m in range(3)]
    norm_train, norm_step = arguments[9:]
    rows, columns = matrices[0].rows, matrices[0].columns
    total_rows = rows * parts

    shifts = sorted(range(1, parts), key=lambda k: -bin(k).count("1"))
    far, near = shifts[:1], shifts[1:]
    first, carrier, last = 0, 1, 2

    whole = cuts_of(rows, [None])
    messages = {
        first: [(cut, far) for cut in cuts_of(rows, [128, 384, None])] + [(whole[0], near)],
        carrier: [(whole[0], shifts)],
        last: [(whole[0], far)] + [(cut, near) for cut in cuts_of(rows, [None, 384, 128])],
    }

    def wire(values, shift):
        return exchange(values, "zero", parts, shift)

    norm = norm_train + norm_step
    norms = [norm] + [exchange(norm, "width", widths, w) for w in range(1, widths)]
    norms = jnp.stack(norms)

    at = 2 * len(matrices)
    extra = -(-(at + widths) // 8) * 8
    sent, sums = {}, {}
    after = matrices[0].high

    def pieces(m, carry=False):
        nonlocal after
        for (start, count), group in messages[m]:
            for shift in group:
                sent[m, shift, start], after = matrices[m].piece(
                    shift, start, count, after, sums.get((m, shift)), extra if carry else 0
                )
                sums[m, shift] = after
                if carry:
                    lines = [sums[o, shift] for o in range(len(matrices))] + [norms]
                    lines += [jnp.zeros((extra - len(matrices) - widths, columns), jnp.float32)]
                    sent[m, shift, start] = matrices[m].carry(
                        sent[m, shift, start], jnp.concatenate(lines), len(matrices), extra
                    )

    pieces(first)
    for m, matrix in enumerate(matrices):
        sums[m, 0] = after = matrix.sums(after)
    pieces(last)
    pieces(carrier, True)

    came = {}
    for m in (first, carrier, last):
        for (start, count), group in messages[m]:
            for shift in group:
                came[m, shift, start] = wire(sent[m, shift, start], shift)

    small = {shift: came[carrier, shift, 0][rows:].astype(jnp.float32) for shift in shifts}
    scales, inverses = [], []
    for m in range(len(matrices)):
        total = sums[m, 0].reshape(columns)
        for shift in shifts:
            total = total + (small[shift][2 * m] + small[shift][2 * m + 1])
        scales.append(total / total_rows)
        inverses.append((1.0 / scales[-1]).reshape(1, columns))

    stack = jnp.stack(
        [norms] + [small[shift][at : at + widths] for shift in range(1, parts)]
    )
    serve_norm = ordered(ordered(stack, place, 0), across, 1).reshape(-1).astype(jnp.bfloat16)

    finals = {}
    after = serve_norm
    for m in (first, carrier, last):
        together, alone = [], []
        for (start, count), group in messages[m]:
            if m != last and count == rows:
                together += [(shift, came[m, shift, start]) for shift in group]
            else:
                alone.append((start, count, group))
        out = matrices[m].own(
            inverses[m], after, [t[1] for t in together], [t[0] for t in together]
        )
        for start, count, group in alone:
            arrived = [came[m, shift, start] for shift in group]
            out = matrices[m].land(out, arrived, inverses[m], group, start, count)
        finals[m] = after = out

    return (finals[0], finals[1], finals[2], *scales, serve_norm)


def by_all_to_all(parts, *arguments):
    finals, scales = [], []
    place = lax.axis_index("zero")
    for m in range(3):
        train, low, high = arguments[3 * m : 3 * m + 3]
        result = train.astype(jnp.float32) + mix_rate * jnp.dot(
            low, high, preferred_element_type=jnp.float32
        )
        total = lax.psum(jnp.sum(jnp.abs(result), axis=0), "zero")
        scale = total / (train.shape[0] * parts)
        narrow = (result / scale).astype(jnp.bfloat16)
        final = lax.all_to_all(narrow, "zero", split_axis=1, concat_axis=0, tiled=True)
        finals.append(final)
        scales.append(lax.dynamic_slice_in_dim(scale, place * final.shape[1], final.shape[1]))
    norm_train, norm_step = arguments[9:]
    serve_norm = lax.all_gather(
        (norm_train + norm_step).astype(jnp.bfloat16), ("zero", "width"), axis=0, tiled=True
    )
    return (*finals, *scales, serve_norm)


def shards(parts, widths, *arguments):
    rows, width = arguments[0].shape
    powers = all(size & (size - 1) == 0 for size in (parts, widths))
    blocks = rows % LANES == 0 and widths <= 8 and width % (parts * LANES) == 0
    if powers and blocks and 1 < parts <= 8:
        return by_permutes(parts, widths, *arguments)
    return by_all_to_all(parts, *arguments)


def solution(mesh):
    weights = (P(("site", "zero"), "width"), P(("site", "zero"), None), P("site", "width"))
    norms = (P(("site", "zero", "width")),) * 2
    out_specs = (
        (P("site", ("width", "zero")),) * 3 + (P(("site", "width", "zero")),) * 3 + (P("site"),)
    )
    body = functools.partial(shards, mesh.shape["zero"], mesh.shape["width"])
    return jax.shard_map(
        body, mesh=mesh, in_specs=weights * 3 + norms, out_specs=out_specs, check_vma=False
    )
```
